32 devices in a mesh: px: 4 (over z), py: 2 (over y), sa: 4 (over x, core).
Axes of the slice: x: 2, y: 2, z: 4, core: 2. Of those that a mesh axis runs over, the one named last changes fastest.
Arguments:
- real_coeffs: float32 [4, 256, 256, 256], P('sa', 'px', 'py'), may hold values from -6 to 6
- imaginary_coeffs: float32 [4, 256, 256, 256], P('sa', 'px', 'py'), may hold values from -6 to 6
Outputs:
- modulus: float32 [4, 256, 256, 256], P(None, ('px', 'py'), 'sa')
The draws below stay inside these ranges and needn't reach their ends.
All inputs are finite; a program needn't handle non-finite values.
Results may differ from the reference program's by a relative error of at most 0.00007.
Values sent between devices are 32-bit elements; how exact they have to be, the bound alone decides.
No kernel may reach another device: no remote copies, remote signals or barrier semaphores. Data moves between devices by JAX's collectives and lax.ppermute only.
A program may use at most 128 MiB of HBM per device.

```python
import math
import jax
import jax.numpy as jnp
from jax import lax

N = 256
SAMPLES = 4


def steps_of(stream_key, extent, pieces, smallest, top_value):
    loudness, own = 1.0, jax.random.fold_in(stream_key, 6)
    for dim, shards_of in pieces:
        steps = jnp.exp(jax.random.uniform(jax.random.fold_in(own, dim), (shards_of,), jnp.float32, smallest / len(pieces), top_value / len(pieces)))
        loudness = loudness * jnp.repeat(steps, extent[dim] // shards_of).reshape([-1 if axis == dim else 1 for axis in range(len(extent))])
    return loudness


def centred(rng, dims, scale, most, cuts=(), held_as=jnp.bfloat16):
    values = jax.random.normal(rng, dims, jnp.float32) * scale
    if len(cuts) > 0:
        values = steps_of(rng, dims, cuts, -0.22, 0.18) * values
    return jnp.clip(values, min=-most, max=most).astype(held_as)


def setup_inputs(seed: int = 0) -> dict:
    key_of = jax.random.split(jax.random.key(seed), 3)
    return {
        "real_coeffs": centred(key_of[0], (SAMPLES, N, N, N), 1.0, 6.0, ((0, 4), (1, 4), (2, 2)), jnp.float32),
        "imaginary_coeffs": centred(key_of[1], (SAMPLES, N, N, N), 1.0, 6.0, ((0, 4), (1, 4), (2, 2)), jnp.float32),
    }


corr_length = 1.0
log_spread = 0.5

def matern(squared, length):
    return 1.0 / (1.0 + (2.0 * math.pi * corr_length / length) ** 2 * squared)

def matern_scale(length):
    middle = length // 2
    square_counts = {}
    for position in range(length):
        square_value = ((position + middle) % length - middle) ** 2
        square_counts[square_value] = square_counts.get(square_value, 0) + 1
    plane_counts = {}
    for first_square, first_count in square_counts.items():
        for second_square, second_count in square_counts.items():
            plane_sum = first_square + second_square
            plane_counts[plane_sum] = plane_counts.get(plane_sum, 0) + first_count * second_count
    running = 0.0
    for first_square, first_count in square_counts.items():
        for plane_sum, plane_count in plane_counts.items():
            running = running + first_count * plane_count * matern(first_square + plane_sum, length) ** 2
    return 1.0 / math.sqrt(running)

def reference(real_coeffs, imaginary_coeffs):
    frequency = ((jnp.arange(N, dtype=jnp.int32) + N // 2) % N - N // 2).astype(jnp.float32)
    squared = frequency[:, None, None] ** 2 + frequency[None, :, None] ** 2 + frequency[None, None, :] ** 2
    weight = matern(squared, N) * matern_scale(N)

    def one_sample(coeff_pair):
        real_part = jnp.transpose(coeff_pair[0], (2, 0, 1))
        imag_part = jnp.transpose(coeff_pair[1], (2, 0, 1))
        spectrum = lax.complex(weight * real_part, weight * imag_part)
        log_field = jnp.real(jnp.fft.ifftn(spectrum)) * float(N ** 3)
        return jnp.exp(log_spread * log_field).astype(jnp.float32)
    return lax.map(one_sample, (real_coeffs, imaginary_coeffs))
```

```python
from functools import partial
import math

import jax
import jax.numpy as jnp
from jax import lax
from jax.sharding import PartitionSpec as P

corr_length = 1.0
log_spread = 0.5


def matern(squared, length):
    return 1.0 / (1.0 + (2.0 * math.pi * corr_length / length) ** 2 * squared)


def matern_scale(length):
    middle = length // 2
    square_counts = {}
    for position in range(length):
        square_value = ((position + middle) % length - middle) ** 2
        square_counts[square_value] = square_counts.get(square_value, 0) + 1
    plane_counts = {}
    for first_square, first_count in square_counts.items():
        for second_square, second_count in square_counts.items():
            plane_sum = first_square + second_square
            plane_counts[plane_sum] = plane_counts.get(plane_sum, 0) + first_count * second_count
    running = 0.0
    for first_square, first_count in square_counts.items():
        for plane_sum, plane_count in plane_counts.items():
            running = (
                running + first_count * plane_count * matern(first_square + plane_sum, length) ** 2
            )
    return 1.0 / math.sqrt(running)


def signed(positions, length):
    return (positions + length // 2) % length - length // 2


def phase_tables(length):
    positions = lax.iota(jnp.int32, length)
    phases = positions[:, None] * positions[None, :] % length
    angles = phases.astype(jnp.float32) * (2.0 * math.pi / length)
    return (jnp.cos(angles), jnp.sin(angles))


def transform(form, tables, pieces):
    cos_table, sin_table = tables
    real_in, imag_in = pieces
    product = partial(jnp.einsum, form, precision=lax.Precision.HIGHEST)
    real_out = product(cos_table, real_in) - product(sin_table, imag_in)
    imag_out = product(sin_table, real_in) + product(cos_table, imag_in)
    return (real_out, imag_out)


def local(real_coeffs, imaginary_coeffs):
    samples, rows_y, rows_z, length = real_coeffs.shape
    across_x = lax.axis_size("px")
    across_y = lax.axis_size("py")
    freq_x = signed(lax.iota(jnp.int32, length), length).astype(jnp.float32)
    freq_y = signed(lax.iota(jnp.int32, rows_y) + lax.axis_index("px") * rows_y, length).astype(
        jnp.float32
    )
    freq_z = signed(lax.iota(jnp.int32, rows_z) + lax.axis_index("py") * rows_z, length).astype(
        jnp.float32
    )
    squared = freq_x[None, None, :] ** 2 + freq_y[:, None, None] ** 2 + freq_z[None, :, None] ** 2
    weight = matern(squared, length) * matern_scale(length)
    tables = phase_tables(length)
    pieces = transform(
        "xk,sabk->sxab", tables, (real_coeffs * weight, imaginary_coeffs * weight)
    )

    def gather(piece):
        block = length // (across_x * across_y)
        shaped = piece.reshape(samples, across_x * across_y, block, rows_y, rows_z)
        moved = lax.all_to_all(shaped, ("px", "py"), split_axis=1, concat_axis=1, tiled=True)
        parted = moved.reshape(samples, across_x, across_y, block, rows_y, rows_z)
        return parted.transpose(0, 3, 1, 4, 2, 5).reshape(samples, block, length, length)

    pieces = transform("yk,sxkq->sxyq", tables, tuple(gather(piece) for piece in pieces))
    product = partial(jnp.einsum, "zk,sxyk->sxyz", precision=lax.Precision.HIGHEST)
    log_field = product(tables[0], pieces[0]) - product(tables[1], pieces[1])
    return lax.all_to_all(
        jnp.exp(log_spread * log_field), "sa", split_axis=2, concat_axis=0, tiled=True
    )


def solution(mesh):
    placed = (P("sa", "px", "py", None), P("sa", "px", "py", None))
    return jax.shard_map(
        local,
        mesh=mesh,
        in_specs=placed,
        out_specs=P(None, ("px", "py"), "sa", None),
        check_vma=False,
    )
```

```python
from functools import partial
import math

import jax
import jax.numpy as jnp
import ml_dtypes
import numpy as np
from jax import lax
from jax.experimental import pallas as pl
from jax.experimental.pallas import tpu as pltpu
from jax.sharding import PartitionSpec as P


corr_length = 1.0
log_spread = 0.5
lane_count = 128
even_shares = (8, 8)
odd_shares = (8, 4, 4)


def matern(squared, length):
    return 1.0 / (1.0 + (2.0 * math.pi * corr_length / length) ** 2 * squared)


def matern_scale(length):
    middle = length // 2
    square_counts = {}
    for position in range(length):
        square_value = ((position + middle) % length - middle) ** 2
        square_counts[square_value] = square_counts.get(square_value, 0) + 1
    plane_counts = {}
    for first_square, first_count in square_counts.items():
        for second_square, second_count in square_counts.items():
            plane_sum = first_square + second_square
            plane_counts[plane_sum] = plane_counts.get(plane_sum, 0) + first_count * second_count
    running = 0.0
    for first_square, first_count in square_counts.items():
        for plane_sum, plane_count in plane_counts.items():
            running = (
                running + first_count * plane_count * matern(first_square + plane_sum, length) ** 2
            )
    return 1.0 / math.sqrt(running)


def signed(positions, length):
    return (positions + length // 2) % length - length // 2


def phase_tables(length):
    positions = lax.iota(jnp.int32, length)
    phases = positions[:, None] * positions[None, :] % length
    angles = phases.astype(jnp.float32) * (2.0 * math.pi / length)
    return (jnp.cos(angles), jnp.sin(angles))


def transform(form, tables, pieces):
    cos_table, sin_table = tables
    real_in, imag_in = pieces
    product = partial(jnp.einsum, form, precision=lax.Precision.HIGHEST)
    real_out = product(cos_table, real_in) - product(sin_table, imag_in)
    imag_out = product(sin_table, real_in) + product(cos_table, imag_in)
    return (real_out, imag_out)


def plain(real_coeffs, imaginary_coeffs):
    samples, rows_y, rows_z, length = real_coeffs.shape
    across_x = lax.axis_size("px")
    across_y = lax.axis_size("py")
    freq_x = signed(lax.iota(jnp.int32, length), length).astype(jnp.float32)
    freq_y = signed(lax.iota(jnp.int32, rows_y) + lax.axis_index("px") * rows_y, length).astype(
        jnp.float32
    )
    freq_z = signed(lax.iota(jnp.int32, rows_z) + lax.axis_index("py") * rows_z, length).astype(
        jnp.float32
    )
    squared = freq_x[None, None, :] ** 2 + freq_y[:, None, None] ** 2 + freq_z[None, :, None] ** 2
    weight = matern(squared, length) * matern_scale(length)
    tables = phase_tables(length)
    pieces = transform(
        "xk,sabk->sxab", tables, (real_coeffs * weight, imaginary_coeffs * weight)
    )

    def gather(piece):
        block = length // (across_x * across_y)
        shaped = piece.reshape(samples, across_x * across_y, block, rows_y, rows_z)
        moved = lax.all_to_all(shaped, ("px", "py"), split_axis=1, concat_axis=1, tiled=True)
        parted = moved.reshape(samples, across_x, across_y, block, rows_y, rows_z)
        return parted.transpose(0, 3, 1, 4, 2, 5).reshape(samples, block, length, length)

    pieces = transform("yk,sxkq->sxyq", tables, tuple(gather(piece) for piece in pieces))
    product = partial(jnp.einsum, "zk,sxyk->sxyz", precision=lax.Precision.HIGHEST)
    log_field = product(tables[0], pieces[0]) - product(tables[1], pieces[1])
    return lax.all_to_all(
        jnp.exp(log_spread * log_field), "sa", split_axis=2, concat_axis=0, tiled=True
    )


def halves(table):
    high = table.astype(ml_dtypes.bfloat16)
    low = (table - high.astype(np.float64)).astype(ml_dtypes.bfloat16)
    return high, low


def waves(length, positions, wave_numbers):
    angles = (positions[:, None] * wave_numbers[None, :] % length) * (2.0 * math.pi / length)
    return np.cos(angles), np.sin(angles)


def x_table(length, blocks, parity, shares):
    block, half = length // blocks, length // 2
    rows, first = [], 0
    for share in shares:
        places = parity + 2 * (first + np.arange(share))
        first += share
        for imaginary in (False, True):
            for place in places:
                rows.append((place, imaginary))
    out = []
    for target in range(blocks):
        places = np.array([target * block + place for place, _ in rows])
        cosine, sine = waves(length, places, np.arange(half))
        real = np.concatenate([cosine, -sine], axis=1)
        imag = np.concatenate([sine, cosine], axis=1)
        out.append(np.where(np.array([flag for _, flag in rows])[:, None], imag, real))
    return np.concatenate(halves(np.stack(out)), axis=2)


def y_table(length, ranks):
    cosine, sine = waves(length, np.arange(length), np.arange(length))
    real = np.concatenate([cosine, -sine], axis=1)
    imag = np.concatenate([sine, cosine], axis=1)
    table = np.stack([real, imag]).reshape(2, ranks, length // ranks, 2 * length)
    return np.concatenate(halves(table), axis=3)


def z_table(length, parts):
    cosine, sine = waves(length, np.arange(length), np.arange(length))
    (cos_high, cos_low), (sin_high, sin_low) = halves(cosine), halves(-sine)
    table = np.stack([cos_high, sin_high, cos_low, sin_low])
    return table.reshape(4, parts, length // parts, length)


def parts_of(values):
    high = values.astype(jnp.bfloat16)
    low = (values - high.astype(jnp.float32)).astype(jnp.bfloat16)
    return high, low


def dot(left, right, contract):
    return lax.dot_general(
        left, right, ((contract[:1], contract[1:]), ((), ())), preferred_element_type=jnp.float32
    )


def x_body(place, real, imag, table, *rest, length, blocks, parity, shares, step_rows, scale):
    outs, kept = rest[:-1], rest[-1]
    me, first_y, first_z = place[0], place[1], place[2]
    half = length // 2
    rows = length // blocks
    rows_z = real.shape[1]

    @pl.when(pl.program_id(0) == 0)
    def _():
        for offset in range(blocks):
            kept[pl.ds(offset * rows, rows), :] = table[me ^ offset]

    table_high, table_low = kept[:, :length], kept[:, length:]
    wave_x = lax.broadcasted_iota(jnp.int32, (1, half), 1)
    wave_z = lax.broadcasted_iota(jnp.int32, (rows_z, 1), 0) + first_z
    near_x = wave_x.astype(jnp.float32)
    far_x = (wave_x - half).astype(jnp.float32)
    freq_z = signed(wave_z, length).astype(jnp.float32)
    factor = (2.0 * math.pi * corr_length / length) ** 2
    group = max(1, length // rows_z)
    for start in range(0, step_rows, group):
        folded = []
        for row in range(start, start + group):
            wave_y = signed(first_y + pl.program_id(0) * step_rows + row, length)
            freq_y = wave_y.astype(jnp.float32)
            near = scale / (1.0 + factor * (near_x * near_x + freq_y * freq_y + freq_z * freq_z))
            far = scale / (1.0 + factor * (far_x * far_x + freq_y * freq_y + freq_z * freq_z))
            pair = []
            for source in (real, imag):
                one = source[row, :, :half] * near
                two = source[row, :, half:] * far
                pair.append(one - two if parity else one + two)
            folded.append(jnp.concatenate(pair, axis=1))
        high, low = parts_of(jnp.concatenate(folded, axis=0))
        result = dot(table_high, high, (1, 1)) + dot(table_high, low, (1, 1))
        result = result + dot(table_low, high, (1, 1))
        for step in range(group):
            piece = result[:, step * rows_z : (step + 1) * rows_z]
            at, number = 0, 0
            for share in shares:
                for offset in range(blocks):
                    begin = offset * rows + at
                    outs[number][:, start + step, :] = piece[begin : begin + 2 * share]
                    number += 1
                at += 2 * share


def x_lines(place, real, imag, table, length, blocks, parity, shares):
    rows_y, rows_z, _ = real.shape
    step_rows = 16
    taken = pl.BlockSpec((step_rows, rows_z, length), lambda g, s: (g, 0, 0))
    shapes, specs = [], []
    for share in shares:
        for _ in range(blocks):
            shapes.append(jax.ShapeDtypeStruct((2 * share, rows_y, rows_z), jnp.float32))
            specs.append(pl.BlockSpec((2 * share, step_rows, rows_z), lambda g, s: (0, g, 0)))
    body = partial(
        x_body, length=length, blocks=blocks, parity=parity, shares=shares, step_rows=step_rows,
        scale=matern_scale(length),
    )
    outs = pl.pallas_call(
        body,
        out_shape=shapes,
        grid_spec=pltpu.PrefetchScalarGridSpec(
            num_scalar_prefetch=1,
            grid=(rows_y // step_rows,),
            in_specs=[taken, taken, pl.BlockSpec(table.shape, lambda g, s: (0, 0, 0))],
            out_specs=specs,
            scratch_shapes=[pltpu.VMEM((length, 2 * length), jnp.bfloat16)],
        ),
        compiler_params=pltpu.CompilerParams(dimension_semantics=("arbitrary",)),
        name=f"x_lines_{parity}",
    )(place, real, imag, table)
    return [outs[n * blocks : (n + 1) * blocks] for n in range(len(shares))]


def yz_body(place, *rest, length, across_x, across_y, ranks):
    blocks = across_x * across_y
    sources, (y_rows, z_rows), rest = rest[:blocks], rest[blocks : blocks + 2], rest[blocks + 2 :]
    outs, (y_kept, z_kept, lines) = rest[:ranks], rest[ranks:]
    me_x, me_y, me_s = place[3], place[4], place[5]
    rows_y, rows_z, own_y = length // across_x, length // across_y, length // ranks

    @pl.when(pl.program_id(0) == 0)
    def _():
        for which in range(2):
            for offset in range(ranks):
                y_kept[pl.ds(which * length + offset * own_y, own_y), :] = y_rows[which, me_s ^ offset]
        for which in range(4):
            for offset in range(across_y):
                z_kept[pl.ds(which * length + offset * rows_z, rows_z), :] = z_rows[which, me_y ^ offset]

    for offset in range(blocks):
        jump_x, jump_y = offset // across_y, offset % across_y
        for which in range(2):
            high, low = parts_of(sources[offset][which, 0])
            at = which * length + (me_x ^ jump_x) * rows_y
            lanes = slice(jump_y * rows_z, (jump_y + 1) * rows_z)
            lines[pl.ds(pl.multiple_of(at, rows_y), rows_y), lanes] = high
            lines[pl.ds(pl.multiple_of(at + 2 * length, rows_y), rows_y), lanes] = low
    high, low = lines[: 2 * length], lines[2 * length :]
    mixed = dot(y_kept[:, : 2 * length], high, (1, 0)) + dot(y_kept[:, : 2 * length], low, (1, 0))
    mixed = mixed + dot(y_kept[:, 2 * length :], high, (1, 0))
    mixed = jnp.concatenate([mixed[:length], mixed[length:]], axis=1)
    high, low = parts_of(mixed)
    field = dot(high, z_kept[: 2 * length], (1, 0)) + dot(low, z_kept[: 2 * length], (1, 0))
    field = field + dot(high, z_kept[2 * length :], (1, 0))
    modulus = jnp.exp(log_spread * field)
    for offset in range(ranks):
        outs[offset][0] = modulus[offset * own_y : (offset + 1) * own_y]


def yz_lines(place, sources, y_rows, z_rows, length, across_x, across_y, ranks):
    share = sources[0].shape[0] // 2
    rows_y, rows_z, own_y = length // across_x, length // across_y, length // ranks
    sources = [source.reshape(2, share, rows_y, rows_z) for source in sources]
    taken = pl.BlockSpec((2, 1, rows_y, rows_z), lambda g, s: (0, g, 0, 0))
    return pl.pallas_call(
        partial(yz_body, length=length, across_x=across_x, across_y=across_y, ranks=ranks),
        out_shape=[jax.ShapeDtypeStruct((share, own_y, length), jnp.float32)] * ranks,
        grid_spec=pltpu.PrefetchScalarGridSpec(
            num_scalar_prefetch=1,
            grid=(share,),
            in_specs=[taken] * len(sources)
            + [
                pl.BlockSpec(y_rows.shape, lambda g, s: (0, 0, 0, 0)),
                pl.BlockSpec(z_rows.shape, lambda g, s: (0, 0, 0, 0)),
            ],
            out_specs=[pl.BlockSpec((1, own_y, length), lambda g, s: (g, 0, 0))] * ranks,
            scratch_shapes=[
                pltpu.VMEM((2 * length, 4 * length), jnp.bfloat16),
                pltpu.VMEM((4 * length, length), jnp.bfloat16),
                pltpu.VMEM((4 * length, length), jnp.bfloat16),
            ],
        ),
        compiler_params=pltpu.CompilerParams(dimension_semantics=("arbitrary",)),
        name="yz_lines",
    )(place, *sources, y_rows, z_rows)


def exchanged(values, axes, sizes, offset):
    count = math.prod(sizes)
    return lax.ppermute(values, axes, [(rank, rank ^ offset) for rank in range(count)])


def pipelined(real_coeffs, imaginary_coeffs):
    _, rows_y, rows_z, length = real_coeffs.shape
    across_x, across_y, ranks = lax.axis_size("px"), lax.axis_size("py"), lax.axis_size("sa")
    blocks = across_x * across_y
    block, own_y = length // blocks, length // ranks
    me_x, me_y, me_s = lax.axis_index("px"), lax.axis_index("py"), lax.axis_index("sa")
    place = jnp.stack(
        [me_x * across_y + me_y, me_x * rows_y, me_y * rows_z, me_x, me_y, me_s]
    ).astype(jnp.int32)
    real, imag = real_coeffs[0], imaginary_coeffs[0]
    y_rows, z_rows = y_table(length, ranks), z_table(length, across_y)
    order = sorted(range(1, blocks), key=lambda offset: -offset)
    out = jnp.zeros((ranks, block // 2, 2, own_y, length), jnp.float32)
    moved = []
    for parity, shares in ((0, even_shares), (1, odd_shares)):
        shares = tuple(share * block // 2 // sum(shares) for share in shares)
        table = x_table(length, blocks, parity, shares)
        first = 0
        for pieces in x_lines(place, real, imag, table, length, blocks, parity, shares):
            arrived = {0: pieces[0]}
            for offset in order:
                arrived[offset] = exchanged(pieces[offset], ("px", "py"), (across_x, across_y), offset)
            moved.append((parity, first, [arrived[offset] for offset in range(blocks)]))
            first += pieces[0].shape[0] // 2
    for parity, first, sources in moved:
        fields = yz_lines(place, sources, y_rows, z_rows, length, across_x, across_y, ranks)
        for offset in range(ranks):
            piece = fields[offset]
            if offset:
                piece = exchanged(piece, ("sa",), (ranks,), offset)
            out = lax.dynamic_update_slice(
                out, piece[None, :, None], (me_s ^ offset, first, parity, 0, 0)
            )
    return out.reshape(ranks, block, own_y, length)


def solution(mesh):
    def local(real_coeffs, imaginary_coeffs):
        samples, rows_y, rows_z, length = real_coeffs.shape
        sizes = [mesh.shape[axis] for axis in ("px", "py", "sa")]
        block = length // (sizes[0] * sizes[1])
        fits = samples == 1 and rows_z % lane_count == 0 and rows_y % 16 == 0
        fits = fits and length % (2 * lane_count) == 0 and block % 32 == 0
        fits = fits and all(size & (size - 1) == 0 for size in sizes)
        return (pipelined if fits else plain)(real_coeffs, imaginary_coeffs)

    placed = (P("sa", "px", "py", None), P("sa", "px", "py", None))
    return jax.shard_map(
        local,
        mesh=mesh,
        in_specs=placed,
        out_specs=P(None, ("px", "py"), "sa", None),
        check_vma=False,
    )
```
